8 devices in a mesh: dp: 1 (over z), ep: 8 (over y, x, core).
Axes of the slice: x: 2, y: 2, z: 1, core: 2. Of those that a mesh axis runs over, the one named last changes fastest.
Arguments:
- hidden_in: bfloat16 [1536, 1536], P(('dp', 'ep'))
- expert_ids: int32 [2, 1536, 8], P(None, ('dp', 'ep'))
- gate_vals: float32 [2, 1536, 8], P(None, ('dp', 'ep'))
- w_gate: bfloat16 [2, 64, 1536, 512], P(None, 'ep')
- w_up: bfloat16 [2, 64, 1536, 512], P(None, 'ep')
- w_down: bfloat16 [2, 64, 512, 1536], P(None, 'ep')
- slot_map: int32 [2, 64], replicated
- slot_moves: int32 [2, 2, 2], replicated
Outputs:
- output 1: bfloat16 [1536, 1536], P(('dp', 'ep'))
- output 2: bfloat16 [2, 64, 1536, 512], P(None, 'ep')
- output 3: bfloat16 [2, 64, 1536, 512], P(None, 'ep')
- output 4: bfloat16 [2, 64, 512, 1536], P(None, 'ep')
All inputs are finite; a program needn't handle non-finite values.
Results may differ from the reference program's by a relative error of at most 0.0149036.
Values are sent between devices in bfloat16 or wider.
A program may use at most 1 GiB of HBM per device.

```python
import jax
import jax.numpy as jnp
from jax import lax

GROUP_SIZE = 8
TOKENS = 192
D_MODEL = 1536
FF_DIM = 512
EXPERTS = 40
TOP_K = 8
SLOTS_DEV = 8
MOVE_COUNT = 2

NUM_SLOTS = GROUP_SIZE * SLOTS_DEV
NUM_ROWS = GROUP_SIZE * TOKENS


def draw_layout(key):
    key_perm, key_extra, key_place = jax.random.split(key, 3)
    expert_perm = jax.random.permutation(key_perm, EXPERTS)
    extra_copies = jax.random.randint(key_extra, (NUM_SLOTS - EXPERTS - MOVE_COUNT,), 0, EXPERTS)
    listing = jnp.concatenate([jnp.arange(EXPERTS), expert_perm[:MOVE_COUNT], extra_copies]).astype(jnp.int32)
    placement = jax.random.permutation(key_place, NUM_SLOTS)
    layout = jnp.zeros((NUM_SLOTS,), jnp.int32).at[placement].set(listing)
    hot_experts = expert_perm[MOVE_COUNT:2 * MOVE_COUNT]
    moves = jnp.stack([placement[EXPERTS:EXPERTS + MOVE_COUNT], placement[hot_experts]]).astype(jnp.int32)
    return layout, moves, hot_experts


def draw_routing(key, hot_experts):
    noise = jax.random.randint(key, (NUM_ROWS, EXPERTS), 0, 1024)
    bonus = jnp.zeros((EXPERTS,), jnp.int32).at[hot_experts].set(512)
    score = (noise + bonus[None, :]) * EXPERTS + jnp.arange(EXPERTS)[None, :]
    return lax.top_k(score, TOP_K)[1].astype(jnp.int32)


def setup_inputs(seed: int = 0, part: int = 0) -> dict:
    key_shared, key_own = jax.random.split(jax.random.key(seed))
    key_own = jax.random.fold_in(key_own, part)
    layer_keys = jax.random.split(key_shared, 3)
    draws = [draw_layout(layer_keys[layer]) for layer in range(2)]
    slot_map = jnp.stack([draws[0][0], draws[1][0]])
    slot_moves = jnp.stack([draws[0][1], draws[1][1]])
    key_wg, key_wu, key_wd = jax.random.split(layer_keys[2], 3)
    expert_gate = jax.random.normal(key_wg, (2, EXPERTS, D_MODEL, FF_DIM), jnp.float32) * D_MODEL ** -0.5
    expert_up = jax.random.normal(key_wu, (2, EXPERTS, D_MODEL, FF_DIM), jnp.float32) * D_MODEL ** -0.5
    expert_down = jax.random.normal(key_wd, (2, EXPERTS, FF_DIM, D_MODEL), jnp.float32) * FF_DIM ** -0.5

    def to_slots(expert_w):
        return jax.vmap(lambda layer_w, layout_row: jnp.take(layer_w, layout_row, axis=0))(expert_w, slot_map).astype(jnp.bfloat16)

    key_x, key_route, key_gate = jax.random.split(key_own, 3)
    route_keys = jax.random.split(key_route, 2)
    expert_ids = jnp.stack([draw_routing(route_keys[layer], draws[layer][2]) for layer in range(2)])
    gate_vals = jax.random.uniform(key_gate, (2, NUM_ROWS, TOP_K), jnp.float32, minval=0.5, maxval=1.5) * TOP_K ** -0.5
    hidden_in = jax.random.normal(key_x, (NUM_ROWS, D_MODEL), jnp.float32).astype(jnp.bfloat16)
    return {"hidden_in": hidden_in, "expert_ids": expert_ids, "gate_vals": gate_vals, "w_gate": to_slots(expert_gate), "w_up": to_slots(expert_up), "w_down": to_slots(expert_down), "slot_map": slot_map, "slot_moves": slot_moves}


def expert_layer(hidden, tok_experts, tok_gates, w_gate, w_up, w_down, layout):
    owner = jnp.argmax(layout[None, :] == jnp.arange(EXPERTS)[:, None], axis=1)
    expert_match = tok_experts[:, :, None] == jnp.arange(EXPERTS)[None, None, :]
    mix_weight = jnp.sum(jnp.where(expert_match, tok_gates[:, :, None], 0.0), axis=1)

    def step(running, inputs):
        wg_e, wu_e, wd_e, mix_col = inputs
        hidden_act = jax.nn.silu(jnp.dot(hidden, wg_e, preferred_element_type=jnp.float32)) * jnp.dot(hidden, wu_e, preferred_element_type=jnp.float32)
        expert_out = jnp.dot(hidden_act.astype(jnp.bfloat16), wd_e, preferred_element_type=jnp.float32).astype(jnp.bfloat16)
        return running + mix_col[:, None] * expert_out.astype(jnp.float32), None

    total, _ = lax.scan(step, jnp.zeros(hidden.shape, jnp.float32), (w_gate[owner], w_up[owner], w_down[owner], mix_weight.T))
    return (hidden.astype(jnp.float32) + total).astype(jnp.bfloat16)


def migrate(weights, moves):
    return weights.at[moves[0]].set(weights[moves[1]])


def reference(hidden_in, expert_ids, gate_vals, w_gate, w_up, w_down, slot_map, slot_moves):
    hidden = hidden_in
    for layer in range(2):
        hidden = expert_layer(hidden, expert_ids[layer], gate_vals[layer], w_gate[layer], w_up[layer], w_down[layer], slot_map[layer])
    new_gate = jnp.stack([migrate(w_gate[layer], slot_moves[layer]) for layer in range(2)])
    new_up = jnp.stack([migrate(w_up[layer], slot_moves[layer]) for layer in range(2)])
    new_down = jnp.stack([migrate(w_down[layer], slot_moves[layer]) for layer in range(2)])
    return hidden, new_gate, new_up, new_down
```

```python
import functools

import jax
import jax.numpy as jnp
from jax import lax
from jax.experimental import pallas as pl
from jax.experimental.pallas import tpu as pltpu
from jax.sharding import PartitionSpec as P


VMEM_LIMIT = 56 * 1024 * 1024


def first_holders(layout):
    index = jnp.arange(layout.shape[0])
    earlier = (index[None, :] < index[:, None]) & (layout[None, :] == layout[:, None])
    return jnp.logical_not(jnp.any(earlier, axis=1))


def half_kernel(chunk, copies, info, *refs):
    blocks, (route, wg, wu, wd) = refs[:8], refs[8:12]
    rest = refs[12 + (3 if copies == 2 else 0):]
    acc = rest[0]
    outs = rest[1:4] if copies else ()
    tokens = rest[-1]
    step = pl.program_id(0)
    rows = blocks[0].shape[0]

    @pl.when(step == 0)
    def _():
        for k in range(8):
            tokens[k * rows:(k + 1) * rows] = blocks[k][...]
        acc[...] = jnp.zeros_like(acc)

    if copies:
        for src, dst in zip((wg, wu, wd), outs):
            dst[...] = src[...]

    @pl.when(info[1 + step] > 0)
    def _():
        column = info[0] + step

        def body(i, carry):
            span = pl.ds(pl.multiple_of(i * chunk, chunk), chunk)
            x = tokens[span]
            gate = jnp.dot(x, wg[0, 0], preferred_element_type=jnp.float32)
            up = jnp.dot(x, wu[0, 0], preferred_element_type=jnp.float32)
            act = (gate * jax.nn.sigmoid(gate) * up).astype(jnp.bfloat16)
            out = jnp.dot(act, wd[0, 0], preferred_element_type=jnp.float32).astype(jnp.bfloat16)
            lanes = route[span]
            lane = lax.broadcasted_iota(jnp.int32, lanes.shape, 1)
            scale = jnp.sum(jnp.where(lane == column, lanes, 0.0), axis=1, keepdims=True)
            acc[span] += scale * out.astype(jnp.float32)
            return carry

        lax.fori_loop(0, tokens.shape[0] // chunk, body, 0)


def half_layer(layer, info, blocks, route, weights, copies, earlier=()):
    w_gate, w_up, w_down = weights
    slots, model, ff = w_gate.shape[1:]
    rows = blocks[0].shape[0]
    chunk = 256
    whole = lambda shape: pl.BlockSpec(shape, lambda s, info: (0,) * len(shape))
    up_spec = pl.BlockSpec((1, 1, model, ff), lambda s, info: (layer, s, 0, 0))
    down_spec = pl.BlockSpec((1, 1, ff, model), lambda s, info: (layer, s, 0, 0))
    wspecs = [up_spec, up_spec, down_spec]
    in_specs = [whole((rows, model))] * 8 + [whole(route.shape)] + wspecs
    out_specs = [whole((8 * rows, model))]
    out_shape = [jax.ShapeDtypeStruct((8 * rows, model), jnp.float32)]
    aliases = {}
    if copies:
        out_specs += wspecs
        out_shape += [jax.ShapeDtypeStruct(w.shape, w.dtype) for w in weights]
    if copies == 2:
        in_specs += [pl.BlockSpec(memory_space=pl.ANY)] * 3
        aliases = {13 + i: 1 + i for i in range(3)}
    nbytes = slots * 3 * model * ff * 2
    return pl.pallas_call(
        functools.partial(half_kernel, chunk, copies),
        grid_spec=pltpu.PrefetchScalarGridSpec(
            num_scalar_prefetch=1,
            grid=(slots,),
            in_specs=in_specs,
            out_specs=out_specs,
            scratch_shapes=[pltpu.VMEM((8 * rows, model), jnp.bfloat16)],
        ),
        out_shape=out_shape,
        input_output_aliases=aliases,
        compiler_params=pltpu.CompilerParams(vmem_limit_bytes=VMEM_LIMIT, dimension_semantics=("arbitrary",)),
        cost_estimate=pl.CostEstimate(flops=slots * 6 * 8 * rows * model * ff, bytes_accessed=nbytes * (2 if copies else 1), transcendentals=0),
        name=f"half_{layer}_{copies}",
    )(info, *blocks, route, *weights, *earlier)


def pick_kernel(info, wg, wu, wd, og, ou, od):
    mine = info[pl.program_id(0), 2] > 0
    for src, dst in ((wg, og), (wu, ou), (wd, od)):
        @pl.when(mine)
        def _():
            dst[...] = src[0]

        @pl.when(jnp.logical_not(mine))
        def _():
            dst[...] = jnp.zeros_like(dst)


def pick_moved(info, weights):
    moves = info.shape[0]
    pick = lambda w: pl.BlockSpec((1, 1) + w.shape[2:], lambda m, info: (info[m, 0], info[m, 1], 0, 0))
    place = lambda w: pl.BlockSpec((1,) + w.shape[2:], lambda m, info: (m, 0, 0))
    return pl.pallas_call(
        pick_kernel,
        grid_spec=pltpu.PrefetchScalarGridSpec(
            num_scalar_prefetch=1, grid=(moves,), in_specs=[pick(w) for w in weights], out_specs=[place(w) for w in weights]
        ),
        out_shape=[jax.ShapeDtypeStruct((moves,) + w.shape[2:], w.dtype) for w in weights],
        compiler_params=pltpu.CompilerParams(vmem_limit_bytes=VMEM_LIMIT),
        name="pick",
    )(info, *weights)


def install_kernel(info, *refs):
    arrived, outs, bufs, sem = refs[:3], refs[6:9], refs[9:12], refs[12]
    for m in range(info.shape[0]):
        @pl.when(info[m, 2] > 0)
        def _():
            loads = [pltpu.make_async_copy(a.at[m], b, sem.at[i]) for i, (a, b) in enumerate(zip(arrived, bufs))]
            stores = [pltpu.make_async_copy(b, o.at[info[m, 0], info[m, 1]], sem.at[3 + i]) for i, (b, o) in enumerate(zip(bufs, outs))]
            for load in loads:
                load.start()
            for load, store in zip(loads, stores):
                load.wait()
                store.start()
            for store in stores:
                store.wait()


def install_moved(info, arrived, new_ws):
    anywhere = pl.BlockSpec(memory_space=pl.ANY)
    return pl.pallas_call(
        install_kernel,
        in_specs=[pl.BlockSpec(memory_space=pltpu.SMEM)] + [anywhere] * 6,
        out_specs=[anywhere] * 3,
        out_shape=[jax.ShapeDtypeStruct(w.shape, w.dtype) for w in new_ws],
        scratch_shapes=[pltpu.VMEM(a.shape[1:], a.dtype) for a in arrived] + [pltpu.SemaphoreType.DMA((6,))],
        input_output_aliases={4 + i: i for i in range(3)},
        compiler_params=pltpu.CompilerParams(vmem_limit_bytes=VMEM_LIMIT),
        name="install",
    )(info, *arrived, *new_ws)


def solution(mesh):
    tok_spec = P(("dp", "ep"), None)
    route_spec = P(None, ("dp", "ep"), None)
    weight_spec = P(None, "ep", None, None)
    count = mesh.shape["ep"]

    def send(value, offset):
        return lax.ppermute(value, "ep", [(r, r ^ offset) for r in range(count)])

    def gather(block):
        near = [block] + [send(block, k) for k in (2, 4, 6)]
        far = [send(b, 1) for b in near]
        return [near[k // 2] if k % 2 == 0 else far[k // 2] for k in range(8)]

    def scatter_sum(partial):
        rows = partial.shape[0] // 8
        block = lambda k: partial[k * rows:(k + 1) * rows]
        pair = [block(k) + send(block(k + 1), 1) for k in (0, 2, 4, 6)]
        return ((pair[0] + send(pair[1], 2)) + send(pair[2], 4)) + send(pair[3], 6)

    def body(hidden_in, expert_ids, gate_vals, w_gate, w_up, w_down, slot_map, slot_moves):
        weights = (w_gate, w_up, w_down)
        slots = w_gate.shape[1]
        half = hidden_in.shape[0] // 2
        rank = lax.axis_index("ep")
        first = jax.vmap(first_holders)(slot_map)

        layer_of = jnp.repeat(jnp.arange(2, dtype=jnp.int32), 2)
        dst, src = slot_moves[:, 0].reshape(-1), slot_moves[:, 1].reshape(-1)
        src_info = jnp.stack([layer_of, src % slots, (src // slots == rank).astype(jnp.int32)], axis=1)
        dst_info = jnp.stack([layer_of, dst % slots, (dst // slots == rank).astype(jnp.int32)], axis=1)
        arrived = lax.psum(tuple(pick_moved(src_info, weights)), "ep")

        holder = jnp.where(first, slot_map, -1)
        match = expert_ids[:, :, :, None] == holder[:, None, None, :]
        by_slot = jnp.sum(jnp.where(match, gate_vals[:, :, :, None], 0.0), axis=2)
        route = jnp.concatenate([by_slot[0], by_slot[1]], axis=1)

        hidden = [hidden_in[:half], hidden_in[half:]]
        routes = [jnp.concatenate(gather(route[:half]), axis=0), jnp.concatenate(gather(route[half:]), axis=0)]
        new_ws = ()
        for layer in range(2):
            active = lax.dynamic_slice(first[layer], (rank * slots,), (slots,)).astype(jnp.int32)
            info = jnp.concatenate([(layer * slots * count + rank * slots).astype(jnp.int32)[None], active])
            for part in range(2):
                blocks = gather(hidden[part])
                copies = 0 if part else 1 + layer
                results = half_layer(layer, info, blocks, routes[part], weights, copies, new_ws if copies == 2 else ())
                if copies:
                    new_ws = tuple(results[1:])
                hidden[part] = (hidden[part].astype(jnp.float32) + scatter_sum(results[0])).astype(jnp.bfloat16)
        new_ws = install_moved(dst_info, arrived, new_ws)
        return (jnp.concatenate(hidden, axis=0),) + tuple(new_ws)

    return jax.shard_map(body, mesh=mesh, in_specs=(tok_spec, route_spec, route_spec, weight_spec, weight_spec, weight_spec, P(None, None), P(None, None, None)), out_specs=(tok_spec, weight_spec, weight_spec, weight_spec), check_vma=False)
```

```python
import functools

import jax
import jax.numpy as jnp
from jax import lax
from jax.experimental import pallas as pl
from jax.experimental.pallas import tpu as pltpu
from jax.sharding import PartitionSpec as P

VMEM_LIMIT = 60 * 1024 * 1024
MESH = pl.DeviceIdType.MESH


def first_holders(layout):
    index = jnp.arange(layout.shape[0])
    earlier = (index[None, :] < index[:, None]) & (layout[None, :] == layout[:, None])
    return jnp.logical_not(jnp.any(earlier, axis=1))


def peers():
    me = lax.axis_index("ep")
    core = me % 2
    across = lambda r, bit: r + bit - 2 * bit * ((r // bit) % 2)
    near_x, near_y = across(me, 2), across(me, 4)
    first = near_x * (1 - core) + near_y * core
    second = near_y * (1 - core) + near_x * core
    return me, across(me, 1), first, second, across(near_x, 4)


def partner_order(partner):
    core = partner % 2
    across = lambda r, bit: r + bit - 2 * bit * ((r // bit) % 2)
    near_x, near_y = across(partner, 2), across(partner, 4)
    first = near_x * (1 - core) + near_y * core
    second = near_y * (1 - core) + near_x * core
    return across(near_x, 4), first, second, partner


def remote(src, dst, sends, recvs, i, rank):
    return pltpu.make_async_remote_copy(src_ref=src, dst_ref=dst, send_sem=sends.at[i], recv_sem=recvs.at[i], device_id={"ep": rank}, device_id_type=MESH)


def greet(ranks):
    barrier = pltpu.get_barrier_semaphore()
    for rank in ranks:
        pl.semaphore_signal(barrier, inc=1, device_id={"ep": rank}, device_id_type=MESH)
    pl.semaphore_wait(barrier, len(ranks))


def spread(table, outs, own, sends, recvs, stores, base):
    me, partner, first, second, opposite = peers()
    rows = own.shape[0]
    at = lambda rank: pl.ds(pl.multiple_of(rank * rows, rows), rows)
    to_first = remote(own, table.at[at(me)], sends, recvs, base, first)
    to_second = remote(own, table.at[at(me)], sends, recvs, base + 1, second)
    to_partner = remote(own, table.at[at(me)], sends, recvs, base + 2, partner)
    to_second.start()
    to_first.start()
    to_partner.start()
    store = lambda i, src, rank: pltpu.make_async_copy(src, outs.at[at(rank)], stores.at[i])
    done = [store(0, own, me)]
    done[0].start()
    to_first.wait_recv()
    forward = remote(table.at[at(first)], table.at[at(first)], sends, recvs, base + 3, second)
    forward.start()
    relays = [remote(table.at[at(first)], table.at[at(first)], sends, recvs, base + 4, partner)]
    relays[0].start()
    done.append(store(1, table.at[at(first)], first))
    done[1].start()
    to_second.wait_recv()
    relays.append(remote(table.at[at(second)], table.at[at(second)], sends, recvs, base + 5, partner))
    relays[1].start()
    done.append(store(2, table.at[at(second)], second))
    done[2].start()
    p_opposite, p_first, p_second, _ = partner_order(partner)
    to_partner.wait_recv()
    done.append(store(3, table.at[at(partner)], partner))
    done[3].start()
    forward.wait_recv()
    relays.append(remote(table.at[at(opposite)], table.at[at(opposite)], sends, recvs, base + 6, partner))
    relays[2].start()
    done.append(store(4, table.at[at(opposite)], opposite))
    done[4].start()
    for i, rank in enumerate((p_first, p_second, p_opposite)):
        relays[i].wait_recv()
        done.append(store(5 + i, table.at[at(rank)], rank))
        done[5 + i].start()
    for copy in [to_first, to_second, to_partner, forward] + relays:
        copy.wait_send()
    for copy in done:
        copy.wait()


def gather_kernel(hidden, route, tokens, routes, table, route_table, sends, recvs, stores, route_sends, route_recvs, route_stores):
    _, partner, first, second, _ = peers()
    greet((partner, first, second))
    spread(table, tokens, hidden, sends, recvs, stores, 0)
    spread(route_table, routes, route, route_sends, route_recvs, route_stores, 0)


def gather_all(hidden, route):
    rows, model = hidden.shape
    lanes = route.shape[1]
    vmem, anywhere = pl.BlockSpec(memory_space=pltpu.VMEM), pl.BlockSpec(memory_space=pl.ANY)
    dma = pltpu.SemaphoreType.DMA
    return pl.pallas_call(
        gather_kernel,
        in_specs=[vmem, vmem],
        out_specs=[anywhere, anywhere],
        out_shape=[jax.ShapeDtypeStruct((8 * rows, model), hidden.dtype), jax.ShapeDtypeStruct((8 * rows, lanes), route.dtype)],
        scratch_shapes=[pltpu.VMEM((8 * rows, model), hidden.dtype), pltpu.VMEM((8 * rows, lanes), route.dtype), dma((7,)), dma((7,)), dma((8,)), dma((7,)), dma((7,)), dma((8,))],
        compiler_params=pltpu.CompilerParams(vmem_limit_bytes=VMEM_LIMIT, collective_id=0, has_side_effects=True),
        name="gather_all",
    )(hidden, route)


def return_kernel(again, partial, hidden, *refs):
    if again:
        result, tokens, mine, theirs, from_first, from_second, table, loads, sends, recvs, stores, sends2, recvs2 = refs
    else:
        result, mine, theirs, from_first, from_second, loads, sends, recvs = refs
    me, partner, first, second, opposite = peers()
    rows = hidden.shape[0]
    at = lambda rank: pl.ds(pl.multiple_of(rank * rows, rows), rows)
    order = (opposite, first, second, me)
    load = [pltpu.make_async_copy(partial.at[at(rank)], mine.at[i], loads.at[i]) for i, rank in enumerate(order)]
    for copy in load:
        copy.start()
    greet((partner, first, second))
    pair = [remote(partial.at[at(rank)], theirs.at[i], sends, recvs, i, partner) for i, rank in enumerate(partner_order(partner))]
    for copy in pair:
        copy.start()
    span = 16

    def add(dst, i, *srcs):
        def body(j, carry):
            s = pl.ds(pl.multiple_of(j * span, span), span)
            total = dst[i, s]
            for src in srcs:
                total = total + src[s]
            dst[i, s] = total
            return carry

        lax.fori_loop(0, rows // span, body, 0)

    out = [remote(mine.at[0], from_first.at[0], sends, recvs, 4, first), remote(mine.at[1], from_first.at[1], sends, recvs, 5, first), remote(mine.at[2], from_second, sends, recvs, 6, second)]
    for i in range(2):
        load[i].wait()
        pair[i].wait_recv()
        add(mine, i, theirs.at[i])
        out[i].start()
    load[2].wait()
    pair[2].wait_recv()
    out[0].wait_recv()
    add(mine, 2, theirs.at[2], from_first.at[0])
    out[2].start()
    load[3].wait()
    pair[3].wait_recv()
    add(mine, 3, theirs.at[3])
    out[1].wait_recv()
    out[2].wait_recv()

    def last(j, carry):
        s = pl.ds(pl.multiple_of(j * span, span), span)
        total = (mine[3, s] + from_first[1, s]) + from_second[s]
        result[s] = (hidden[s].astype(jnp.float32) + total).astype(result.dtype)
        return carry

    lax.fori_loop(0, rows // span, last, 0)
    for copy in pair + out:
        copy.wait_send()
    if again:
        spread(table, tokens, result, sends2, recvs2, stores, 0)


def return_sum(partial, hidden, again):
    rows, model = hidden.shape
    vmem, anywhere = pl.BlockSpec(memory_space=pltpu.VMEM), pl.BlockSpec(memory_space=pl.ANY)
    dma = pltpu.SemaphoreType.DMA
    block = lambda n: pltpu.VMEM((n, rows, model), jnp.float32)
    scratch = [block(4), block(4), block(2), pltpu.VMEM((rows, model), jnp.float32)]
    if again:
        scratch += [pltpu.VMEM((8 * rows, model), hidden.dtype), dma((4,)), dma((7,)), dma((7,)), dma((8,)), dma((7,)), dma((7,))]
    else:
        scratch += [dma((4,)), dma((7,)), dma((7,))]
    out_shape = [jax.ShapeDtypeStruct((rows, model), hidden.dtype)]
    if again:
        out_shape.append(jax.ShapeDtypeStruct((8 * rows, model), hidden.dtype))
    return pl.pallas_call(
        functools.partial(return_kernel, again),
        in_specs=[anywhere, vmem],
        out_specs=[vmem, anywhere][: len(out_shape)],
        out_shape=out_shape,
        scratch_shapes=scratch,
        compiler_params=pltpu.CompilerParams(vmem_limit_bytes=VMEM_LIMIT, collective_id=1 + int(again), has_side_effects=True),
        name="return_gather" if again else "return_last",
    )(partial, hidden)


def layer_kernel(chunk, chained, info, *refs):
    tokens, route, wg, wu, wd = refs[:5]
    acc, og, ou, od = refs[5 + (3 if chained else 0):]
    step = pl.program_id(0)

    @pl.when(step == 0)
    def _():
        acc[...] = jnp.zeros_like(acc)

    for src, dst in ((wg, og), (wu, ou), (wd, od)):
        dst[...] = src[...]

    @pl.when(info[1 + step] > 0)
    def _():
        column = info[0] + step

        def body(i, carry):
            span = pl.ds(pl.multiple_of(i * chunk, chunk), chunk)
            x = tokens[span]
            gate = jnp.dot(x, wg[0, 0], preferred_element_type=jnp.float32)
            up = jnp.dot(x, wu[0, 0], preferred_element_type=jnp.float32)
            act = (gate * jax.nn.sigmoid(gate) * up).astype(jnp.bfloat16)
            out = jnp.dot(act, wd[0, 0], preferred_element_type=jnp.float32).astype(jnp.bfloat16)
            lanes = route[span]
            lane = lax.broadcasted_iota(jnp.int32, lanes.shape, 1)
            scale = jnp.sum(jnp.where(lane == column, lanes, 0.0), axis=1, keepdims=True)
            acc[span] += scale * out.astype(jnp.float32)
            return carry

        lax.fori_loop(0, tokens.shape[0] // chunk, body, 0)


def layer_sums(layer, info, tokens, route, weights, earlier=()):
    w_gate = weights[0]
    slots, model, ff = w_gate.shape[1:]
    rows = tokens.shape[0]
    whole = lambda shape: pl.BlockSpec(shape, lambda s, info: (0,) * len(shape))
    up_spec = pl.BlockSpec((1, 1, model, ff), lambda s, info: (layer, s, 0, 0))
    down_spec = pl.BlockSpec((1, 1, ff, model), lambda s, info: (layer, s, 0, 0))
    wspecs = [up_spec, up_spec, down_spec]
    chained = bool(earlier)
    nbytes = slots * 3 * model * ff * 2
    return pl.pallas_call(
        functools.partial(layer_kernel, 256, chained),
        grid_spec=pltpu.PrefetchScalarGridSpec(
            num_scalar_prefetch=1,
            grid=(slots,),
            in_specs=[whole(tokens.shape), whole(route.shape)] + wspecs + [pl.BlockSpec(memory_space=pl.ANY)] * len(earlier),
            out_specs=[whole((rows, model))] + wspecs,
        ),
        out_shape=[jax.ShapeDtypeStruct((rows, model), jnp.float32)] + [jax.ShapeDtypeStruct(w.shape, w.dtype) for w in weights],
        input_output_aliases={6 + i: 1 + i for i in range(len(earlier))},
        compiler_params=pltpu.CompilerParams(vmem_limit_bytes=VMEM_LIMIT, dimension_semantics=("arbitrary",)),
        cost_estimate=pl.CostEstimate(flops=slots * 6 * rows * model * ff, bytes_accessed=nbytes * 2, transcendentals=0),
        name=f"layer_{layer}",
    )(info, tokens, route, *weights, *earlier)


def pick_kernel(info, wg, wu, wd, og, ou, od):
    mine = info[pl.program_id(0), 2] > 0
    for src, dst in ((wg, og), (wu, ou), (wd, od)):
        @pl.when(mine)
        def _():
            dst[...] = src[0]

        @pl.when(jnp.logical_not(mine))
        def _():
            dst[...] = jnp.zeros_like(dst)


def pick_moved(info, weights):
    moves = info.shape[0]
    pick = lambda w: pl.BlockSpec((1, 1) + w.shape[2:], lambda m, info: (info[m, 0], info[m, 1], 0, 0))
    place = lambda w: pl.BlockSpec((1,) + w.shape[2:], lambda m, info: (m, 0, 0))
    return pl.pallas_call(
        pick_kernel,
        grid_spec=pltpu.PrefetchScalarGridSpec(
            num_scalar_prefetch=1, grid=(moves,), in_specs=[pick(w) for w in weights], out_specs=[place(w) for w in weights]
        ),
        out_shape=[jax.ShapeDtypeStruct((moves,) + w.shape[2:], w.dtype) for w in weights],
        compiler_params=pltpu.CompilerParams(vmem_limit_bytes=VMEM_LIMIT),
        name="pick",
    )(info, *weights)


def install_kernel(info, *refs):
    arrived, outs, bufs, sem = refs[:3], refs[6:9], refs[9:12], refs[12]
    for m in range(info.shape[0]):
        @pl.when(info[m, 2] > 0)
        def _():
            loads = [pltpu.make_async_copy(a.at[m], b, sem.at[i]) for i, (a, b) in enumerate(zip(arrived, bufs))]
            stores = [pltpu.make_async_copy(b, o.at[info[m, 0], info[m, 1]], sem.at[3 + i]) for i, (b, o) in enumerate(zip(bufs, outs))]
            for load in loads:
                load.start()
            for load, store in zip(loads, stores):
                load.wait()
                store.start()
            for store in stores:
                store.wait()


def install_moved(info, arrived, new_ws):
    anywhere = pl.BlockSpec(memory_space=pl.ANY)
    return pl.pallas_call(
        install_kernel,
        in_specs=[pl.BlockSpec(memory_space=pltpu.SMEM)] + [anywhere] * 6,
        out_specs=[anywhere] * 3,
        out_shape=[jax.ShapeDtypeStruct(w.shape, w.dtype) for w in new_ws],
        scratch_shapes=[pltpu.VMEM(a.shape[1:], a.dtype) for a in arrived] + [pltpu.SemaphoreType.DMA((6,))],
        input_output_aliases={4 + i: i for i in range(3)},
        compiler_params=pltpu.CompilerParams(vmem_limit_bytes=VMEM_LIMIT),
        name="install",
    )(info, *arrived, *new_ws)


def solution(mesh):
    tok_spec = P(("dp", "ep"), None)
    route_spec = P(None, ("dp", "ep"), None)
    weight_spec = P(None, "ep", None, None)
    count = mesh.shape["ep"]

    def body(hidden_in, expert_ids, gate_vals, w_gate, w_up, w_down, slot_map, slot_moves):
        weights = (w_gate, w_up, w_down)
        slots = w_gate.shape[1]
        rank = lax.axis_index("ep")
        first = jax.vmap(first_holders)(slot_map)

        layer_of = jnp.repeat(jnp.arange(2, dtype=jnp.int32), 2)
        dst, src = slot_moves[:, 0].reshape(-1), slot_moves[:, 1].reshape(-1)
        src_info = jnp.stack([layer_of, src % slots, (src // slots == rank).astype(jnp.int32)], axis=1)
        dst_info = jnp.stack([layer_of, dst % slots, (dst // slots == rank).astype(jnp.int32)], axis=1)
        picked = tuple(pick_moved(src_info, weights))
        picked, hidden_in = lax.optimization_barrier((picked, hidden_in))
        arrived = lax.psum(picked, "ep")

        holder = jnp.where(first, slot_map, -1)
        match = expert_ids[:, :, :, None] == holder[:, None, None, :]
        by_slot = jnp.sum(jnp.where(match, gate_vals[:, :, :, None], 0.0), axis=2)
        route = jnp.concatenate([by_slot[0], by_slot[1]], axis=1)

        infos = []
        for layer in range(2):
            active = lax.dynamic_slice(first[layer], (rank * slots,), (slots,)).astype(jnp.int32)
            infos.append(jnp.concatenate([(layer * slots * count + rank * slots).astype(jnp.int32)[None], active]))
        tokens, routes = gather_all(hidden_in, route)
        partial, *new_ws = layer_sums(0, infos[0], tokens, routes, weights)
        hidden, tokens = return_sum(partial, hidden_in, True)
        partial, *new_ws = layer_sums(1, infos[1], tokens, routes, weights, tuple(new_ws))
        (hidden,) = return_sum(partial, hidden, False)
        new_ws = install_moved(dst_info, arrived, new_ws)
        return (hidden,) + tuple(new_ws)

    return jax.shard_map(body, mesh=mesh, in_specs=(tok_spec, route_spec, route_spec, weight_spec, weight_spec, weight_spec, P(None, None), P(None, None, None)), out_specs=(tok_spec, weight_spec, weight_spec, weight_spec), check_vma=False)
```

```python
import functools

import jax
import jax.numpy as jnp
from jax import lax
from jax.experimental import pallas as pl
from jax.experimental.pallas import tpu as pltpu
from jax.sharding import PartitionSpec as P

VMEM_LIMIT = 60 * 1024 * 1024
MESH = pl.DeviceIdType.MESH


QUARTER = 1152


def plan_kernel(rank_ref, layout, moves, holder, table, count, owner, load):
    rank = rank_ref[0]
    slots = layout.shape[1]
    per_dev = slots // 8
    for layer in range(2):
        for d in range(8):
            load[d] = 0

        def clear(e, carry):
            owner[e] = -1
            return carry

        lax.fori_loop(0, owner.shape[0], clear, 0)

        def claim(q, carry):
            e = layout[layer, q]

            @pl.when(owner[e] < 0)
            def _():
                owner[e] = q
                load[q // per_dev] = load[q // per_dev] + 1

            return carry

        lax.fori_loop(0, slots, claim, 0)

        def improve(i, carry):
            q = i % slots
            e = layout[layer, q]
            old, new = owner[e] // per_dev, q // per_dev

            @pl.when(load[new] + 1 < load[old])
            def _():
                owner[e] = q
                load[new] = load[new] + 1
                load[old] = load[old] - 1

            return carry

        lax.fori_loop(0, 3 * slots, improve, 0)

        def publish(q, carry):
            e = layout[layer, q]
            holder[layer, q] = jnp.where(owner[e] == q, e, -1)
            return carry

        lax.fori_loop(0, slots, publish, 0)

    ring_place = lambda chip: 2 * (chip // 2) + (chip % 2 + chip // 2) % 2
    total = jnp.int32(0)
    crosses = []
    for m in range(4):
        dst, src = moves[m // 2, 0, m % 2], moves[m // 2, 1, m % 2]
        crosses.append((dst // per_dev // 2 != src // per_dev // 2).astype(jnp.int32))
        total = total + crosses[-1]
    count[0] = total
    step = jnp.where(total == 1, QUARTER // 8, QUARTER // 18)
    far, near = jnp.int32(0), total
    for m in range(4):
        dst, src = moves[m // 2, 0, m % 2], moves[m // 2, 1, m % 2]
        src_dev, dst_dev = src // per_dev, dst // per_dev
        row = jnp.where(crosses[m] > 0, far, near)
        far, near = far + crosses[m], near + 1 - crosses[m]
        hops = (ring_place(rank // 2) - ring_place(src_dev // 2) + 4) % 4
        src_chip = (src_dev // 2 == rank // 2).astype(jnp.int32)
        fields = [
            jnp.int32(m // 2), src % per_dev, (src_dev == rank).astype(jnp.int32), dst % per_dev, (dst_dev == rank).astype(jnp.int32),
            src_chip, jnp.maximum(hops - 1, 0) * step, jnp.maximum(3 - hops, 0) * step,
        ]
        for f, value in enumerate(fields):
            table[row, f] = value


def make_plan(rank, slot_map, slot_moves):
    smem = pl.BlockSpec(memory_space=pltpu.SMEM)
    return pl.pallas_call(
        plan_kernel,
        in_specs=[smem] * 3,
        out_specs=[smem] * 3,
        out_shape=[jax.ShapeDtypeStruct(slot_map.shape, jnp.int32), jax.ShapeDtypeStruct((4, 8), jnp.int32), jax.ShapeDtypeStruct((1,), jnp.int32)],
        scratch_shapes=[pltpu.SMEM((64,), jnp.int32), pltpu.SMEM((8,), jnp.int32)],
        name="plan",
    )(rank, slot_map, slot_moves)


def peers():
    me = lax.axis_index("ep")
    core = me % 2
    across = lambda r, bit: r + bit - 2 * bit * ((r // bit) % 2)
    near_x, near_y = across(me, 2), across(me, 4)
    first = near_x * (1 - core) + near_y * core
    second = near_y * (1 - core) + near_x * core
    return me, across(me, 1), first, second, across(near_x, 4)


def partner_order(partner):
    core = partner % 2
    across = lambda r, bit: r + bit - 2 * bit * ((r // bit) % 2)
    near_x, near_y = across(partner, 2), across(partner, 4)
    first = near_x * (1 - core) + near_y * core
    second = near_y * (1 - core) + near_x * core
    return across(near_x, 4), first, second, partner


def remote(src, dst, sends, recvs, i, rank):
    return pltpu.make_async_remote_copy(src_ref=src, dst_ref=dst, send_sem=sends.at[i], recv_sem=recvs.at[i], device_id={"ep": rank}, device_id_type=MESH)


def greet(ranks):
    barrier = pltpu.get_barrier_semaphore()
    for rank in ranks:
        pl.semaphore_signal(barrier, inc=1, device_id={"ep": rank}, device_id_type=MESH)
    pl.semaphore_wait(barrier, len(ranks))


def spread(table, outs, own, sends, recvs, stores, base):
    me, partner, first, second, opposite = peers()
    rows = own.shape[0]
    at = lambda rank: pl.ds(pl.multiple_of(rank * rows, rows), rows)
    to_first = remote(own, table.at[at(me)], sends, recvs, base, first)
    to_second = remote(own, table.at[at(me)], sends, recvs, base + 1, second)
    to_partner = remote(own, table.at[at(me)], sends, recvs, base + 2, partner)
    to_second.start()
    to_first.start()
    to_partner.start()
    store = lambda i, src, rank: pltpu.make_async_copy(src, outs.at[at(rank)], stores.at[i])
    done = [store(0, own, me)]
    done[0].start()
    to_first.wait_recv()
    forward = remote(table.at[at(first)], table.at[at(first)], sends, recvs, base + 3, second)
    forward.start()
    relays = [remote(table.at[at(first)], table.at[at(first)], sends, recvs, base + 4, partner)]
    relays[0].start()
    done.append(store(1, table.at[at(first)], first))
    done[1].start()
    to_second.wait_recv()
    relays.append(remote(table.at[at(second)], table.at[at(second)], sends, recvs, base + 5, partner))
    relays[1].start()
    done.append(store(2, table.at[at(second)], second))
    done[2].start()
    p_opposite, p_first, p_second, _ = partner_order(partner)
    to_partner.wait_recv()
    done.append(store(3, table.at[at(partner)], partner))
    done[3].start()
    forward.wait_recv()
    relays.append(remote(table.at[at(opposite)], table.at[at(opposite)], sends, recvs, base + 6, partner))
    relays[2].start()
    done.append(store(4, table.at[at(opposite)], opposite))
    done[4].start()
    for i, rank in enumerate((p_first, p_second, p_opposite)):
        relays[i].wait_recv()
        done.append(store(5 + i, table.at[at(rank)], rank))
        done[5 + i].start()
    for copy in [to_first, to_second, to_partner, forward] + relays:
        copy.wait_send()
    for copy in done:
        copy.wait()


def gather_kernel(hidden, route, tokens, routes, table, route_table, sends, recvs, stores, route_sends, route_recvs, route_stores):
    _, partner, first, second, _ = peers()
    greet((partner, first, second))
    spread(table, tokens, hidden, sends, recvs, stores, 0)
    spread(route_table, routes, route, route_sends, route_recvs, route_stores, 0)


def gather_all(hidden, route):
    rows, model = hidden.shape
    lanes = route.shape[1]
    vmem, anywhere = pl.BlockSpec(memory_space=pltpu.VMEM), pl.BlockSpec(memory_space=pl.ANY)
    dma = pltpu.SemaphoreType.DMA
    return pl.pallas_call(
        gather_kernel,
        in_specs=[vmem, vmem],
        out_specs=[anywhere, anywhere],
        out_shape=[jax.ShapeDtypeStruct((8 * rows, model), hidden.dtype), jax.ShapeDtypeStruct((8 * rows, lanes), route.dtype)],
        scratch_shapes=[pltpu.VMEM((8 * rows, model), hidden.dtype), pltpu.VMEM((8 * rows, lanes), route.dtype), dma((7,)), dma((7,)), dma((8,)), dma((7,)), dma((7,)), dma((8,))],
        compiler_params=pltpu.CompilerParams(vmem_limit_bytes=VMEM_LIMIT, collective_id=0, has_side_effects=True),
        name="gather_all",
    )(hidden, route)


def return_kernel(again, partial, hidden, *refs):
    if again:
        result, tokens, mine, theirs, from_first, from_second, table, loads, sends, recvs, stores, sends2, recvs2 = refs
    else:
        result, mine, theirs, from_first, from_second, loads, sends, recvs = refs
    me, partner, first, second, opposite = peers()
    rows = hidden.shape[0]
    at = lambda rank: pl.ds(pl.multiple_of(rank * rows, rows), rows)
    order = (opposite, first, second, me)
    load = [pltpu.make_async_copy(partial.at[at(rank)], mine.at[i], loads.at[i]) for i, rank in enumerate(order)]
    for copy in load:
        copy.start()
    greet((partner, first, second))
    pair = [remote(partial.at[at(rank)], theirs.at[i], sends, recvs, i, partner) for i, rank in enumerate(partner_order(partner))]
    for copy in pair:
        copy.start()
    span = 16

    def add(dst, i, *srcs):
        def body(j, carry):
            s = pl.ds(pl.multiple_of(j * span, span), span)
            total = dst[i, s]
            for src in srcs:
                total = total + src[s]
            dst[i, s] = total
            return carry

        lax.fori_loop(0, rows // span, body, 0)

    out = [remote(mine.at[0], from_first.at[0], sends, recvs, 4, first), remote(mine.at[1], from_first.at[1], sends, recvs, 5, first), remote(mine.at[2], from_second, sends, recvs, 6, second)]
    for i in range(2):
        load[i].wait()
        pair[i].wait_recv()
        add(mine, i, theirs.at[i])
        out[i].start()
    load[2].wait()
    pair[2].wait_recv()
    out[0].wait_recv()
    add(mine, 2, theirs.at[2], from_first.at[0])
    out[2].start()
    load[3].wait()
    pair[3].wait_recv()
    add(mine, 3, theirs.at[3])
    out[1].wait_recv()
    out[2].wait_recv()

    def last(j, carry):
        s = pl.ds(pl.multiple_of(j * span, span), span)
        total = (mine[3, s] + from_first[1, s]) + from_second[s]
        result[s] = (hidden[s].astype(jnp.float32) + total).astype(result.dtype)
        return carry

    lax.fori_loop(0, rows // span, last, 0)
    for copy in pair + out:
        copy.wait_send()
    if again:
        spread(table, tokens, result, sends2, recvs2, stores, 0)


def return_sum(partial, hidden, again):
    rows, model = hidden.shape
    vmem, anywhere = pl.BlockSpec(memory_space=pltpu.VMEM), pl.BlockSpec(memory_space=pl.ANY)
    dma = pltpu.SemaphoreType.DMA
    block = lambda n: pltpu.VMEM((n, rows, model), jnp.float32)
    scratch = [block(4), block(4), block(2), pltpu.VMEM((rows, model), jnp.float32)]
    if again:
        scratch += [pltpu.VMEM((8 * rows, model), hidden.dtype), dma((4,)), dma((7,)), dma((7,)), dma((8,)), dma((7,)), dma((7,))]
    else:
        scratch += [dma((4,)), dma((7,)), dma((7,))]
    out_shape = [jax.ShapeDtypeStruct((rows, model), hidden.dtype)]
    if again:
        out_shape.append(jax.ShapeDtypeStruct((8 * rows, model), hidden.dtype))
    return pl.pallas_call(
        functools.partial(return_kernel, again),
        in_specs=[anywhere, vmem],
        out_specs=[vmem, anywhere][: len(out_shape)],
        out_shape=out_shape,
        scratch_shapes=scratch,
        compiler_params=pltpu.CompilerParams(vmem_limit_bytes=VMEM_LIMIT, collective_id=1 + int(again), has_side_effects=True),
        name="return_gather" if again else "return_last",
    )(partial, hidden)


def layer_kernel(chunk, chained, info, *refs):
    tokens, route, wg, wu, wd = refs[:5]
    acc, og, ou, od = refs[5 + (3 if chained else 0):]
    step = pl.program_id(0)

    @pl.when(step == 0)
    def _():
        acc[...] = jnp.zeros_like(acc)

    for src, dst in ((wg, og), (wu, ou), (wd, od)):
        dst[...] = src[...]

    @pl.when(info[1 + step] > 0)
    def _():
        column = info[0] + step

        def body(i, carry):
            span = pl.ds(pl.multiple_of(i * chunk, chunk), chunk)
            x = tokens[span]
            gate = jnp.dot(x, wg[0, 0], preferred_element_type=jnp.float32)
            up = jnp.dot(x, wu[0, 0], preferred_element_type=jnp.float32)
            act = (gate * jax.nn.sigmoid(gate) * up).astype(jnp.bfloat16)
            out = jnp.dot(act, wd[0, 0], preferred_element_type=jnp.float32).astype(jnp.bfloat16)
            lanes = route[span]
            lane = lax.broadcasted_iota(jnp.int32, lanes.shape, 1)
            scale = jnp.sum(jnp.where(lane == column, lanes, 0.0), axis=1, keepdims=True)
            acc[span] += scale * out.astype(jnp.float32)
            return carry

        lax.fori_loop(0, tokens.shape[0] // chunk, body, 0)


def layer_sums(layer, info, tokens, route, weights, earlier=()):
    w_gate = weights[0]
    slots, model, ff = w_gate.shape[1:]
    rows = tokens.shape[0]
    whole = lambda shape: pl.BlockSpec(shape, lambda s, info: (0,) * len(shape))
    up_spec = pl.BlockSpec((1, 1, model, ff), lambda s, info: (layer, s, 0, 0))
    down_spec = pl.BlockSpec((1, 1, ff, model), lambda s, info: (layer, s, 0, 0))
    wspecs = [up_spec, up_spec, down_spec]
    chained = bool(earlier)
    nbytes = slots * 3 * model * ff * 2
    return pl.pallas_call(
        functools.partial(layer_kernel, 256, chained),
        grid_spec=pltpu.PrefetchScalarGridSpec(
            num_scalar_prefetch=1,
            grid=(slots,),
            in_specs=[whole(tokens.shape), whole(route.shape)] + wspecs + [pl.BlockSpec(memory_space=pl.ANY)] * len(earlier),
            out_specs=[whole((rows, model))] + wspecs,
        ),
        out_shape=[jax.ShapeDtypeStruct((rows, model), jnp.float32)] + [jax.ShapeDtypeStruct(w.shape, w.dtype) for w in weights],
        input_output_aliases={6 + i: 1 + i for i in range(len(earlier))},
        compiler_params=pltpu.CompilerParams(vmem_limit_bytes=VMEM_LIMIT, dimension_semantics=("arbitrary",)),
        cost_estimate=pl.CostEstimate(flops=slots * 6 * rows * model * ff, bytes_accessed=nbytes * 2, transcendentals=0),
        name=f"layer_{layer}",
    )(info, tokens, route, *weights, *earlier)


def pick_kernel(table, wg, wu, wd, og, ou, od):
    @pl.when(table[pl.program_id(0), 2] > 0)
    def _():
        for src, dst in ((wg, og), (wu, ou), (wd, od)):
            dst[...] = src[0]


def pick_moved(table, weights):
    moves = table.shape[0]

    def source(m, t):
        mine = t[m, 2]
        return (t[m, 0] * mine, t[m, 1] * mine, 0, 0)

    pick = lambda w: pl.BlockSpec((1, 1) + w.shape[2:], source)
    place = lambda w: pl.BlockSpec((1,) + w.shape[2:], lambda m, t: (jnp.where(t[m, 2] > 0, m, moves), 0, 0))
    return pl.pallas_call(
        pick_kernel,
        grid_spec=pltpu.PrefetchScalarGridSpec(
            num_scalar_prefetch=1, grid=(moves,), in_specs=[pick(w) for w in weights], out_specs=[place(w) for w in weights]
        ),
        out_shape=[jax.ShapeDtypeStruct((moves + 1,) + w.shape[2:], w.dtype) for w in weights],
        compiler_params=pltpu.CompilerParams(vmem_limit_bytes=VMEM_LIMIT),
        name="pick",
    )(table, *weights)


def merge_kernel(table, core, ag, au, ad, bg, bu, bd, out):
    m = pl.program_id(0)
    third, ff = ag.shape[1:]
    lanes = out.shape[3]
    for mine, (g, u, d) in ((1, (ag, au, ad)), (0, (bg, bu, bd))):
        @pl.when((table[m, 5] > 0) & (table[m, 2] == mine))
        def _():
            out[0, 0, 0:third] = g[0]
            out[0, 0, third:2 * third] = u[0]
            rows = d.shape[1]
            for i in range(d.shape[2] // lanes):
                out[0, 0, 2 * third + i * rows:2 * third + (i + 1) * rows] = d[0, :, i * lanes:(i + 1) * lanes]


def merge_picked(table, core, picked, partner):
    moves = table.shape[0]
    model, ff = picked[0].shape[1:]

    def quarter(mine):
        def index(m, way, t, c):
            used = t[m, 5] * (t[m, 2] if mine else 1 - t[m, 2])
            return (m * used, (2 * way + c[0]) * used, 0)

        return index

    specs = lambda mine: [pl.BlockSpec((1, w.shape[1] // 4, w.shape[2]), quarter(mine)) for w in picked]
    return pl.pallas_call(
        merge_kernel,
        grid_spec=pltpu.PrefetchScalarGridSpec(
            num_scalar_prefetch=2,
            grid=(moves, 2),
            in_specs=specs(True) + specs(False),
            out_specs=pl.BlockSpec((1, 1, QUARTER, ff), lambda m, way, t, c: (jnp.where(t[m, 5] > 0, m, moves), way * t[m, 5], 0, 0)),
        ),
        out_shape=jax.ShapeDtypeStruct((moves + 1, 2, QUARTER, ff), picked[0].dtype),
        compiler_params=pltpu.CompilerParams(vmem_limit_bytes=VMEM_LIMIT),
        name="merge",
    )(table, core, *picked, *partner)


def ring_kernel(n, pieces, table, own, landed, relayed, own_v, land, out_v, loads, sends, recvs, stores, relay_sends, relay_recvs):
    me = lax.axis_index("ep")
    core, chip = me % 2, me // 2
    x, y = chip % 2, chip // 2
    ahead = 2 * (2 * x + 1 - y) + core
    behind = 2 * (2 * (1 - x) + y) + core
    partner = me + 1 - 2 * core
    to = (ahead, behind)
    rows = QUARTER // pieces
    rounds = pieces + 2
    pairs = [(m, way) for m in range(n) for way in range(2)]
    load = [pltpu.make_async_copy(own.at[m, way], own_v.at[m, way], loads.at[m, way]) for m, way in pairs]
    for copy in load:
        copy.start()
    greet((ahead, behind, partner))
    for copy in load:
        copy.wait()
    at = lambda k: pl.ds(pl.multiple_of(k * rows, 16), rows)

    def hop(m, way, k):
        return pltpu.make_async_remote_copy(
            src_ref=out_v.at[k % 2, m, way], dst_ref=land.at[m, way, at(k)], send_sem=sends.at[k % 2, m, way],
            recv_sem=recvs.at[k, m, way], device_id={"ep": to[way]}, device_id_type=MESH)

    def emit(k, fresh):
        for m, way in pairs:
            mine = own_v[m, way, at(jnp.minimum(k, pieces - 1))]
            if fresh:
                out_v[k % 2, m, way] = mine
            else:
                hop(m, way, k - 1).wait_recv()
                out_v[k % 2, m, way] = jnp.where(table[m, 5] > 0, mine, land[m, way, at(k - 1)])
            hop(m, way, k).start()

    emit(0, True)
    emit(1, False)

    def body(k, carry):
        for m, way in pairs:
            hop(m, way, k - 2).wait_send()
        emit(k, False)
        return carry

    pending = []

    def publish(g, low, high):
        span = pl.ds(low * rows, (high - low) * rows)
        for m, way in pairs:
            store = pltpu.make_async_copy(land.at[m, way, span], landed.at[m, way, span], stores.at[g, m, way])
            relay = pltpu.make_async_remote_copy(
                src_ref=land.at[m, way, span], dst_ref=relayed.at[m, way, span], send_sem=relay_sends.at[g, m, way],
                recv_sem=relay_recvs.at[g, m, way], device_id={"ep": partner}, device_id_type=MESH)
            store.start()
            relay.start()
            pending.append((store, relay))

    middle = rounds // 2
    lax.fori_loop(2, middle, body, 0)
    publish(0, 0, middle - 1)
    lax.fori_loop(middle, rounds, body, 0)
    for m, way in pairs:
        hop(m, way, rounds - 1).wait_recv()
    publish(1, middle - 1, rounds)
    for m, way in pairs:
        hop(m, way, rounds - 2).wait_send()
        hop(m, way, rounds - 1).wait_send()
    for store, relay in pending:
        store.wait()
        relay.wait()


LAND_ROWS = 10 * (QUARTER // 8)


def run_ring(n, table, own):
    ff = own.shape[3]
    shape = jax.ShapeDtypeStruct((4, 2, LAND_ROWS, ff), own.dtype)
    pieces = 8 if n == 1 else 18
    rows, rounds = QUARTER // pieces, pieces + 2
    dma = pltpu.SemaphoreType.DMA
    anywhere = pl.BlockSpec(memory_space=pl.ANY)
    landed, relayed = pl.pallas_call(
        functools.partial(ring_kernel, n, pieces),
        in_specs=[pl.BlockSpec(memory_space=pltpu.SMEM), anywhere],
        out_specs=[anywhere] * 2,
        out_shape=[shape] * 2,
        scratch_shapes=[
            pltpu.VMEM((n, 2, QUARTER, ff), own.dtype), pltpu.VMEM((n, 2, rounds * rows, ff), own.dtype), pltpu.VMEM((2, n, 2, rows, ff), own.dtype),
            dma((n, 2)), dma((2, n, 2)), dma((rounds, n, 2)), dma((2, n, 2)), dma((2, n, 2)), dma((2, n, 2)),
        ],
        compiler_params=pltpu.CompilerParams(vmem_limit_bytes=VMEM_LIMIT, collective_id=2 + n, has_side_effects=True),
        name=f"ring_{n}",
    )(table, own)
    return landed, relayed


def install_kernel(table, core, *refs):
    here, partner, (landed, relayed), outs = refs[:3], refs[3:6], refs[6:8], refs[11:14]
    bufs, sem = refs[14:17], refs[17]
    lanes = landed.shape[3]
    for m in range(table.shape[0]):
        mine, local = table[m, 4] > 0, table[m, 5] > 0

        def fill(copies):
            for copy in copies:
                copy.start()
            for copy in copies:
                copy.wait()

        for own, arrays in ((1, here), (0, partner)):
            @pl.when(mine & local & (table[m, 2] == own))
            def _():
                fill([pltpu.make_async_copy(a.at[m], b, sem.at[i]) for i, (a, b) in enumerate(zip(arrays, bufs))])

        @pl.when(mine & jnp.logical_not(local))
        def _():
            for c, arrays in ((0, (landed, relayed)), (1, (relayed, landed))):
                @pl.when(core[0] == c)
                def _():
                    copies = []
                    for way in range(2):
                        for which in range(2):
                            src = arrays[which].at[m, way]
                            base = pl.multiple_of(table[m, 6 + way], 16)
                            q = 2 * way + which
                            for i in range(2):
                                rows = bufs[i].shape[0] // 4
                                copies.append((src.at[pl.ds(base + i * rows, rows)], bufs[i].at[pl.ds(q * rows, rows)]))
                            skip = 2 * (bufs[0].shape[0] // 4)
                            rows = bufs[2].shape[0] // 4
                            for i in range(bufs[2].shape[1] // lanes):
                                copies.append((src.at[pl.ds(base + skip + i * rows, rows)], bufs[2].at[pl.ds(q * rows, rows), pl.ds(i * lanes, lanes)]))
                    fill([pltpu.make_async_copy(a, b, sem.at[i]) for i, (a, b) in enumerate(copies)])

        @pl.when(mine)
        def _():
            fill([pltpu.make_async_copy(b, o.at[table[m, 0], table[m, 3]], sem.at[i]) for i, (b, o) in enumerate(zip(bufs, outs))])


def install_moved(table, core, picked, partner, ring, new_ws):
    anywhere, smem = pl.BlockSpec(memory_space=pl.ANY), pl.BlockSpec(memory_space=pltpu.SMEM)
    return pl.pallas_call(
        install_kernel,
        in_specs=[smem] * 2 + [anywhere] * 11,
        out_specs=[anywhere] * 3,
        out_shape=[jax.ShapeDtypeStruct(w.shape, w.dtype) for w in new_ws],
        scratch_shapes=[pltpu.VMEM(w.shape[2:], w.dtype) for w in new_ws] + [pltpu.SemaphoreType.DMA((20,))],
        input_output_aliases={10 + i: i for i in range(3)},
        compiler_params=pltpu.CompilerParams(vmem_limit_bytes=VMEM_LIMIT),
        name="install",
    )(table, core, *picked, *partner, *ring, *new_ws)


def solution(mesh):
    tok_spec = P(("dp", "ep"), None)
    route_spec = P(None, ("dp", "ep"), None)
    weight_spec = P(None, "ep", None, None)
    count = mesh.shape["ep"]

    def body(hidden_in, expert_ids, gate_vals, w_gate, w_up, w_down, slot_map, slot_moves):
        weights = (w_gate, w_up, w_down)
        slots = w_gate.shape[1]
        rank = lax.axis_index("ep").astype(jnp.int32)
        core = (rank % 2)[None]
        holder, table, crossing = make_plan(rank[None], slot_map, slot_moves)

        picked = pick_moved(table, weights)
        partner = [lax.ppermute(p, "ep", [(r, r ^ 1) for r in range(count)]) for p in picked]
        own = merge_picked(table, core, picked, partner)
        nothing = jnp.zeros((4, 2, LAND_ROWS, own.shape[3]), own.dtype)
        ring = lax.switch(crossing[0], [lambda t, o: (nothing, nothing)] + [functools.partial(run_ring, n) for n in range(1, 5)], table, own)

        match = expert_ids[:, :, :, None] == holder[:, None, None, :]
        by_slot = jnp.sum(jnp.where(match, gate_vals[:, :, :, None], 0.0), axis=2)
        route = jnp.concatenate([by_slot[0], by_slot[1]], axis=1)

        infos = []
        for layer in range(2):
            active = (lax.dynamic_slice(holder[layer], (rank * slots,), (slots,)) >= 0).astype(jnp.int32)
            infos.append(jnp.concatenate([(layer * slots * count + rank * slots)[None], active]))
        tokens, routes = gather_all(hidden_in, route)
        partial, *new_ws = layer_sums(0, infos[0], tokens, routes, weights)
        hidden, tokens = return_sum(partial, hidden_in, True)
        partial, *new_ws = layer_sums(1, infos[1], tokens, routes, weights, tuple(new_ws))
        (hidden,) = return_sum(partial, hidden, False)
        new_ws = install_moved(table, core, picked, partner, ring, new_ws)
        return (hidden,) + tuple(new_ws)

    return jax.shard_map(body, mesh=mesh, in_specs=(tok_spec, route_spec, route_spec, weight_spec, weight_spec, weight_spec, P(None, None), P(None, None, None)), out_specs=(tok_spec, weight_spec, weight_spec, weight_spec), check_vma=False)
```
